128 devices in a mesh: gx: 8 (over z, core), gy: 16 (over x, y).
Axes of the slice: x: 4, y: 4, z: 4, core: 2. Of those that a mesh axis runs over, the one named last changes fastest.
Arguments:
- policy_logp: float32 [16, 2048, 4096], P('gy', 'gx'), may hold values from -2 to 0
- anchor_logp: float32 [16, 2048, 4096], P('gy', 'gx'), may hold values from -2 to 0
- lengths: int32 [16, 2048], P('gy', 'gx'), may hold values from 512 to 4096
- rewards: int32 [16, 2048], P('gy', 'gx'), may hold values from 0 to 8
- slot_prompt: int32 [16, 2048], P('gy', 'gx'), may hold values from 0 to 2047, as said below
Outputs:
- token_grad: float32 [16, 2048, 4096], P(None, ('gx', 'gy'))
- sample_loss: float32 [16, 2048], P(None, ('gx', 'gy'))
- advantage: float32 [16, 2048], P(None, ('gx', 'gy'))
The draws below stay inside these ranges and needn't reach their ends.
Inputs may be any that keep to these rules, and one draw needn't show every extreme that they name: `slot_prompt`: for every member k and every aligned block of 256 slots, the slots of the block hold each prompt of the same block exactly once.
All inputs are finite; a program needn't handle non-finite values.
Results may differ from the reference program's by a relative error of at most 0.00002.
Values sent between devices are 32-bit elements; how exact they have to be, the bound alone decides.
A program may use at most 64 MiB of HBM per device.

```python
import jax
import jax.numpy as jnp

K = 16
LMAX = 4096
PROMPTS = 2048
BLOCK = 256
SAMPLES = 32768
N_GX = 8


def draw_slot_prompt(key, part):
    subkeys = jax.random.split(jax.random.fold_in(key, 7), K * N_GX)
    shuffled = jax.vmap(lambda subkey: jax.random.permutation(subkey, BLOCK))(subkeys)
    shuffled = shuffled.astype(jnp.int32).reshape(K, N_GX, BLOCK)
    offsets = (jnp.arange(N_GX, dtype=jnp.int32) * BLOCK)[None, :, None]
    return (shuffled + offsets).reshape(K, PROMPTS).astype(jnp.int32)


def with_ends(values, stream_key, least, high):
    spot = [jax.random.randint(jax.random.fold_in(stream_key, axis), (), 0, length) for axis, length in enumerate(values.shape)]
    widest = values.shape.index(max(values.shape))
    neighbour = spot[:widest] + [(spot[widest] + 1) % values.shape[widest]] + spot[widest + 1:]
    return values.at[tuple(spot)].set(least).at[tuple(neighbour)].set(high)


def level_of(stream_key, shape, cuts, low, top_value):
    level, own = 1.0, jax.random.fold_in(stream_key, 6)
    for dim, shards_of in cuts:
        steps = jnp.exp(jax.random.uniform(jax.random.fold_in(own, dim), (shards_of,), jnp.float32, low / len(cuts), top_value / len(cuts)))
        level = level * jnp.repeat(steps, shape[dim] // shards_of).reshape([-1 if axis == dim else 1 for axis in range(len(shape))])
    return level


def setup_inputs(seed: int = 0) -> dict:
    key_list = jax.random.split(jax.random.key(seed), 6)
    policy_logp = jnp.clip(-2.0 + 2.0 * jax.random.uniform(key_list[0], (K, PROMPTS, LMAX), jnp.float32) ** level_of(key_list[0], (K, PROMPTS, LMAX), ((0, 16), (1, 8)), -0.2, 0.2), -2.0, 0.0)
    anchor_logp = jnp.clip(-2.0 + 2.0 * jax.random.uniform(key_list[1], (K, PROMPTS, LMAX), jnp.float32) ** level_of(key_list[1], (K, PROMPTS, LMAX), ((0, 16), (1, 8)), -0.2, 0.2), -2.0, 0.0)
    lengths = with_ends(jax.random.randint(key_list[2], (K, PROMPTS), LMAX // 8, LMAX + 1), jax.random.fold_in(key_list[2], 1), LMAX // 8, LMAX).astype(jnp.int32)
    rewards = with_ends(jax.random.randint(key_list[3], (K, PROMPTS), 0, 9), jax.random.fold_in(key_list[3], 1), 0, 8).astype(jnp.int32)
    slot_prompt = draw_slot_prompt(jax.random.fold_in(key_list[5], 71), 0)
    return dict(policy_logp=policy_logp, anchor_logp=anchor_logp, lengths=lengths, rewards=rewards, slot_prompt=slot_prompt)


kl_weight = 0.1


def reference(policy_logp, anchor_logp, lengths, rewards, slot_prompt):
    member_rows = jnp.arange(K, dtype=jnp.int32)[:, None]
    slot_ids = jnp.broadcast_to(jnp.arange(PROMPTS, dtype=jnp.int32)[None, :], (K, PROMPTS))
    inverse = jnp.zeros((K, PROMPTS), jnp.int32).at[member_rows, slot_prompt].set(slot_ids)
    policy = jnp.take_along_axis(policy_logp, inverse[:, :, None], axis=1)
    anchor = jnp.take_along_axis(anchor_logp, inverse[:, :, None], axis=1)
    seq_len = jnp.take_along_axis(lengths, inverse, axis=1)
    reward = jnp.take_along_axis(rewards, inverse, axis=1).astype(jnp.float32) * 0.25
    total = jnp.sum(reward, axis=0)
    advantage = (K * reward - total[None, :]) / (K - 1)
    ntok = jnp.sum(lengths).astype(jnp.float32)
    positions = jnp.arange(LMAX, dtype=jnp.int32)[None, None, :]
    valid = positions < seq_len[:, :, None]
    log_ratio = anchor - policy
    ratio = jnp.exp(log_ratio)
    token_term = -advantage[:, :, None] * policy + kl_weight * (ratio - log_ratio - 1.0)
    token_grad = jnp.where(valid, -advantage[:, :, None] + kl_weight * (1.0 - ratio), 0.0) * (SAMPLES * LMAX / ntok)
    sample_loss = jnp.sum(jnp.where(valid, token_term, 0.0), axis=2) * (SAMPLES / ntok)
    return token_grad, sample_loss, advantage
```

```python
import functools

import jax
import jax.numpy as jnp
from jax import lax
from jax.experimental import pallas as pl
from jax.experimental.pallas import tpu as pltpu
from jax.sharding import Mesh
from jax.sharding import PartitionSpec as P

GX_GY = ("gx_0", "gx_1", "gy_0", "gy_1")
GY = ("gy_0", "gy_1")
GX = ("gx_0", "gx_1")
MESH = pl.DeviceIdType.MESH

MEMBERS = 16
SLOTS = 256
TOKENS = 4096
SAMPLES = 32768
KL = 0.1
CHUNKS = 8
WIDTH = TOKENS // CHUNKS
LANES = 128

OFFSETS = (
    (2, 2), (2, 1), (1, 2), (2, 3), (3, 2), (1, 1), (3, 3), (1, 3),
    (3, 1), (0, 2), (2, 0), (0, 1), (1, 0), (0, 3), (3, 0),
)
GX_OFFSETS = ((2, 1), (2, 0), (1, 1), (3, 1), (1, 0), (3, 0), (0, 1))


def parts_of(x):
    high = x.astype(jnp.bfloat16)
    rest = x - high.astype(jnp.float32)
    mid = rest.astype(jnp.bfloat16)
    low = (rest - mid.astype(jnp.float32)).astype(jnp.bfloat16)
    return high, mid, low


def picked(x, one_hot, contract):
    dims = (((1,), (contract,)), ((), ()))
    high, mid, low = (
        lax.dot_general(part, one_hot, dims, preferred_element_type=jnp.float32)
        for part in parts_of(x)
    )
    return (high + mid) + low


def kernel(
    policy_hbm, anchor_hbm, len_ref, reward_ref, prompt_ref,
    grad_ref, loss_ref, adv_ref,
    policy, anchor, stack, one_hot3, sent, got, sums, len_col,
    info_out, info_in, sums_out, sums_in, count_out, count_in, len_in, adv_in,
    load_sem, send_sem, recv_sem, info_send, info_recv, sums_send, sums_recv, count_send, count_recv,
):
    mz, mc = lax.axis_index("gx_0"), lax.axis_index("gx_1")
    mx, my = lax.axis_index("gy_0"), lax.axis_index("gy_1")
    me = mx * 4 + my
    me_gx = mz * 2 + mc

    def peer(dx, dy):
        return lax.rem(mx + dx, 4), lax.rem(my + dy, 4)

    def loads(ch):
        cols = pl.ds(pl.multiple_of(ch * WIDTH, WIDTH), WIDTH)
        return (
            pltpu.make_async_copy(policy_hbm.at[:, cols], policy.at[:, cols], load_sem.at[0, ch]),
            pltpu.make_async_copy(anchor_hbm.at[:, cols], anchor.at[:, cols], load_sem.at[1, ch]),
        )

    barrier = pltpu.get_barrier_semaphore()
    for dx, dy in OFFSETS:
        px, py = peer(dx, dy)
        pl.semaphore_signal(barrier, inc=1, device_id=(mz, mc, px, py), device_id_type=MESH)
    for dz, dc in GX_OFFSETS:
        pl.semaphore_signal(
            barrier, inc=1, device_id=(lax.rem(mz + dz, 4), lax.rem(mc + dc, 2), mx, my), device_id_type=MESH
        )
    for ch in range(CHUNKS):
        for copy in loads(ch):
            copy.start()

    local_prompt = jnp.bitwise_and(prompt_ref[...], SLOTS - 1)
    rows = lax.broadcasted_iota(jnp.int32, (SLOTS, SLOTS), 0)
    lanes = lax.broadcasted_iota(jnp.int32, (SLOTS, SLOTS), 1)
    hot = jnp.where(rows == local_prompt, 1.0, 0.0).astype(jnp.bfloat16)
    for part in range(3):
        one_hot3[:, part * SLOTS : (part + 1) * SLOTS] = hot
    lens = len_ref[...].astype(jnp.float32)
    rewards = reward_ref[...].astype(jnp.float32) * 0.25
    column = jnp.sum(jnp.where(rows == lanes, lens, 0.0), axis=1, keepdims=True)
    len_col[...] = jnp.broadcast_to(column, (SLOTS, LANES))
    which = lax.broadcasted_iota(jnp.int32, (8, SLOTS), 0)
    both = jnp.where(which == 0, lens, jnp.where(which == 1, rewards, 0.0))
    moved = picked(both, hot, 1)
    local_count = jnp.sum(lens, axis=1, keepdims=True)
    for half in range(2):
        at = half * LANES
        info_out[half, 0:2, :] = moved[0:2, at : at + LANES]
        info_out[half, 2:4, :] = jnp.broadcast_to(local_count, (2, LANES))
    sums[...] = jnp.zeros_like(sums)

    def compute(ch):
        for copy in loads(ch):
            copy.wait()

        @pl.loop(0, SLOTS // 16)
        def _(block):
            r0 = pl.multiple_of(block * 16, 16)
            length = len_col[pl.ds(r0, 16), :]
            s1 = sums[0, pl.ds(r0, 16), :]
            s2 = sums[1, pl.ds(r0, 16), :]
            lane = lax.broadcasted_iota(jnp.int32, (16, LANES), 1)
            for t in range(WIDTH // LANES):
                c0 = pl.multiple_of(ch * WIDTH + t * LANES, LANES)
                p = policy[pl.ds(r0, 16), pl.ds(c0, LANES)]
                a = anchor[pl.ds(r0, 16), pl.ds(c0, LANES)]
                valid = (lane + c0).astype(jnp.float32) < length
                d = a - p
                ratio = jnp.exp(d)
                s1 = s1 + jnp.where(valid, p, 0.0)
                s2 = s2 + jnp.where(valid, ratio - d - 1.0, 0.0)
                for i, part in enumerate(parts_of(ratio)):
                    stack[pl.ds(pl.multiple_of(i * SLOTS + r0, 16), 16), t * LANES : (t + 1) * LANES] = part
            sums[0, pl.ds(r0, 16), :] = s1
            sums[1, pl.ds(r0, 16), :] = s2

        cols = pl.ds(pl.multiple_of(ch * WIDTH, WIDTH), WIDTH)
        sent[:, cols] = jnp.dot(one_hot3[...], stack[...], preferred_element_type=jnp.float32)
        got[me, :, cols] = sent[pl.ds(pl.multiple_of(me * 16, 16), 16), cols]

    def copies(ch):
        cols = pl.ds(pl.multiple_of(ch * WIDTH, WIDTH), WIDTH)
        for j, (dx, dy) in enumerate(OFFSETS):
            px, py = peer(dx, dy)
            first = pl.multiple_of((px * 4 + py) * 16, 16)
            yield pltpu.make_async_remote_copy(
                src_ref=sent.at[pl.ds(first, 16), cols],
                dst_ref=got.at[me, :, cols],
                send_sem=send_sem.at[ch, j],
                recv_sem=recv_sem.at[ch, j],
                device_id=(mz, mc, px, py),
                device_id_type=MESH,
            )

    def small_copies(source, target, sends, recvs):
        for j, (dx, dy) in enumerate(OFFSETS):
            px, py = peer(dx, dy)
            yield pltpu.make_async_remote_copy(
                src_ref=source.at[lax.div(px, 2)],
                dst_ref=target.at[me],
                send_sem=sends.at[j],
                recv_sem=recvs.at[j],
                device_id=(mz, mc, px, py),
                device_id_type=MESH,
            )

    def count_copies():
        for j, (dz, dc) in enumerate(GX_OFFSETS):
            yield pltpu.make_async_remote_copy(
                src_ref=count_out,
                dst_ref=count_in.at[me_gx],
                send_sem=count_send.at[j],
                recv_sem=count_recv.at[j],
                device_id=(lax.rem(mz + dz, 4), lax.rem(mc + dc, 2), mx, my),
                device_id_type=MESH,
            )

    compute(0)
    pl.semaphore_wait(barrier, len(OFFSETS) + len(GX_OFFSETS))
    for copy in small_copies(info_out, info_in, info_send, info_recv):
        copy.start()
    for copy in copies(0):
        copy.start()

    @pl.loop(1, CHUNKS - 1)
    def _(ch):
        compute(ch)
        for copy in copies(ch):
            copy.start()

    compute(CHUNKS - 1)
    ones = jnp.ones((8, LANES), jnp.float32)
    across = (((1,), (1,)), ((), ()))
    row1, row2 = (
        lax.dot_general(ones, sums[i], across, precision=lax.Precision.HIGHEST, preferred_element_type=jnp.float32)
        for i in range(2)
    )
    moved = picked(jnp.where(which == 0, row1, row2), hot, 1)
    for half in range(2):
        at = half * LANES
        sums_out[half] = moved[0:2, at : at + LANES]
    for copy in small_copies(sums_out, sums_in, sums_send, sums_recv):
        copy.start()
    for copy in copies(CHUNKS - 1):
        copy.start()

    half = lax.div(mx, 2)
    info_in[me] = info_out[half]
    sums_in[me] = sums_out[half]
    for copy in small_copies(info_out, info_in, info_send, info_recv):
        copy.wait()
    count = info_in[0, 2:3, :]
    for k in range(1, MEMBERS):
        count = count + info_in[k, 2:3, :]
    count_out[...] = count
    count_in[me_gx] = count
    for copy in count_copies():
        copy.start()

    total = info_in[0, 1:2, :]
    for k in range(1, MEMBERS):
        total = total + info_in[k, 1:2, :]
    lane = lax.broadcasted_iota(jnp.int32, (16, LANES), 1)
    row = lax.broadcasted_iota(jnp.int32, (16, LANES), 0)
    mine = lane == lax.rem(me, 8) * 16 + row

    def to_column(line):
        return jnp.broadcast_to(jnp.sum(jnp.where(mine, line, 0.0), axis=1, keepdims=True), (16, LANES))

    for k in range(MEMBERS):
        advantage = (MEMBERS * info_in[k, 1:2, :] - total) / (MEMBERS - 1)
        len_in[k] = to_column(info_in[k, 0:1, :])
        adv_in[k] = to_column(advantage)

    for copy in count_copies():
        copy.wait()
    tokens = count_in[0]
    for g in range(1, 8):
        tokens = tokens + count_in[g]
    grad_scale = SAMPLES * TOKENS / tokens
    loss_scale = SAMPLES / tokens

    @pl.loop(0, CHUNKS)
    def _(ch):
        for copy in copies(ch):
            copy.wait_recv()

        @pl.loop(0, MEMBERS)
        def _(k):
            length = len_in[k]
            advantage = adv_in[k]
            for t in range(WIDTH // LANES):
                c0 = pl.multiple_of(ch * WIDTH + t * LANES, LANES)
                ratio = got[k, :, pl.ds(c0, LANES)]
                valid = (lane + c0).astype(jnp.float32) < length
                grad_ref[k, :, pl.ds(c0, LANES)] = (
                    jnp.where(valid, KL * (1.0 - ratio) - advantage, 0.0) * grad_scale
                )

    for copy in small_copies(sums_out, sums_in, sums_send, sums_recv):
        copy.wait()
    member = lax.broadcasted_iota(jnp.int32, (MEMBERS, LANES), 0)
    adv_rows = jnp.zeros((MEMBERS, LANES), jnp.float32)
    loss_rows = jnp.zeros((MEMBERS, LANES), jnp.float32)
    for k in range(MEMBERS):
        advantage = (MEMBERS * info_in[k, 1:2, :] - total) / (MEMBERS - 1)
        loss = (KL * sums_in[k, 1:2, :] - advantage * sums_in[k, 0:1, :]) * loss_scale
        adv_rows = jnp.where(member == k, advantage, adv_rows)
        loss_rows = jnp.where(member == k, loss, loss_rows)
    select = jnp.where(mine, 1.0, 0.0).astype(jnp.bfloat16)
    loss_ref[...] = picked(loss_rows, select, 1)
    adv_ref[...] = picked(adv_rows, select, 1)

    @pl.loop(0, CHUNKS)
    def _(ch):
        for copy in copies(ch):
            copy.wait_send()


def body(policy_logp, anchor_logp, lengths, rewards, slot_prompt):
    f32, bf16, dma = jnp.float32, jnp.bfloat16, pltpu.SemaphoreType.DMA
    n = len(OFFSETS)
    vmem = pl.BlockSpec(memory_space=pltpu.VMEM)
    hbm = pl.BlockSpec(memory_space=pl.ANY)
    return pl.pallas_call(
        kernel,
        out_shape=(
            pltpu.VMEM((MEMBERS, 16, TOKENS), f32),
            pltpu.VMEM((MEMBERS, 16), f32),
            pltpu.VMEM((MEMBERS, 16), f32),
        ),
        in_specs=[hbm, hbm, vmem, vmem, vmem],
        out_specs=(vmem, vmem, vmem),
        scratch_shapes=[
            pltpu.VMEM((SLOTS, TOKENS), f32),
            pltpu.VMEM((SLOTS, TOKENS), f32),
            pltpu.VMEM((3 * SLOTS, WIDTH), bf16),
            pltpu.VMEM((SLOTS, 3 * SLOTS), bf16),
            pltpu.VMEM((SLOTS, TOKENS), f32),
            pltpu.VMEM((MEMBERS, 16, TOKENS), f32),
            pltpu.VMEM((2, SLOTS, LANES), f32),
            pltpu.VMEM((SLOTS, LANES), f32),
            pltpu.VMEM((2, 4, LANES), f32),
            pltpu.VMEM((MEMBERS, 4, LANES), f32),
            pltpu.VMEM((2, 2, LANES), f32),
            pltpu.VMEM((MEMBERS, 2, LANES), f32),
            pltpu.VMEM((1, LANES), f32),
            pltpu.VMEM((8, 1, LANES), f32),
            pltpu.VMEM((MEMBERS, 16, LANES), f32),
            pltpu.VMEM((MEMBERS, 16, LANES), f32),
            dma((2, CHUNKS)), dma((CHUNKS, n)), dma((CHUNKS, n)),
            dma((n,)), dma((n,)), dma((n,)), dma((n,)),
            dma((len(GX_OFFSETS),)), dma((len(GX_OFFSETS),)),
        ],
        compiler_params=pltpu.CompilerParams(
            collective_id=0, has_side_effects=True, vmem_limit_bytes=50 * 2**20
        ),
    )(policy_logp.reshape(SLOTS, TOKENS), anchor_logp.reshape(SLOTS, TOKENS), lengths, rewards, slot_prompt)


def solution(mesh):
    torus = Mesh(mesh.devices.reshape(4, 2, 4, 4), ("gx_0", "gx_1", "gy_0", "gy_1"))
    return jax.shard_map(
        body,
        mesh=torus,
        in_specs=(P(GY, GX, None), P(GY, GX, None), P(GY, GX), P(GY, GX), P(GY, GX)),
        out_specs=(P(None, GX_GY, None), P(None, GX_GY), P(None, GX_GY)),
        check_vma=False,
    )
```

```python
import functools

import jax
import jax.numpy as jnp
from jax import lax
from jax.experimental import pallas as pl
from jax.experimental.pallas import tpu as pltpu
from jax.sharding import Mesh
from jax.sharding import PartitionSpec as P

GX_GY = ("gx_0", "gx_1", "gy_0", "gy_1")
GY = ("gy_0", "gy_1")
GX = ("gx_0", "gx_1")
MESH = pl.DeviceIdType.MESH

MEMBERS = 16
SLOTS = 256
TOKENS = 4096
SAMPLES = 32768
KL = 0.1
LANES = 128
UNIT = 256
WIDTHS = (256, 512, 768, 1024, 1024, 512)
STARTS = tuple(sum(WIDTHS[:i]) for i in range(len(WIDTHS)))
CHUNKS = len(WIDTHS)

OFFSETS = (
    (2, 2), (2, 1), (1, 2), (2, 3), (3, 2), (1, 1), (3, 3), (1, 3),
    (3, 1), (0, 2), (2, 0), (0, 1), (1, 0), (0, 3), (3, 0),
)
GX_OFFSETS = ((2, 1), (2, 0), (1, 1), (3, 1), (1, 0), (3, 0), (0, 1))


def parts_of(x):
    high = x.astype(jnp.bfloat16)
    rest = x - high.astype(jnp.float32)
    mid = rest.astype(jnp.bfloat16)
    low = (rest - mid.astype(jnp.float32)).astype(jnp.bfloat16)
    return high, mid, low


def picked(x, one_hot, contract):
    dims = (((1,), (contract,)), ((), ()))
    high, mid, low = (
        lax.dot_general(part, one_hot, dims, preferred_element_type=jnp.float32)
        for part in parts_of(x)
    )
    return (high + mid) + low


def kernel(
    policy_hbm, anchor_hbm, len_hbm, reward_hbm, prompt_hbm,
    grad_ref, loss_ref, adv_ref,
    policy, anchor, facts, stack, one_hot3, sent, got, sums, len_col,
    info_out, info_in, sums_out, sums_in, count_out, count_in, len_in, adv_in,
    load_sem, facts_sem, send_sem, recv_sem,
    info_send, info_recv, sums_send, sums_recv, count_send, count_recv,
):
    mz, mc = lax.axis_index("gx_0"), lax.axis_index("gx_1")
    mx, my = lax.axis_index("gy_0"), lax.axis_index("gy_1")
    me = mx * 4 + my
    me_gx = mz * 2 + mc

    def peer(dx, dy):
        return lax.rem(mx + dx, 4), lax.rem(my + dy, 4)

    def columns(ch):
        return pl.ds(STARTS[ch], WIDTHS[ch])

    def loads(ch):
        cols = columns(ch)
        return (
            pltpu.make_async_copy(policy_hbm.at[:, cols], policy.at[:, cols], load_sem.at[0, ch]),
            pltpu.make_async_copy(anchor_hbm.at[:, cols], anchor.at[:, cols], load_sem.at[1, ch]),
        )

    fact_loads = [
        pltpu.make_async_copy(source, facts.at[i], facts_sem.at[i])
        for i, source in enumerate((prompt_hbm, len_hbm, reward_hbm))
    ]

    barrier = pltpu.get_barrier_semaphore()
    for dx, dy in OFFSETS:
        px, py = peer(dx, dy)
        pl.semaphore_signal(barrier, inc=1, device_id=(mz, mc, px, py), device_id_type=MESH)
    for dz, dc in GX_OFFSETS:
        pl.semaphore_signal(
            barrier, inc=1, device_id=(lax.rem(mz + dz, 4), lax.rem(mc + dc, 2), mx, my), device_id_type=MESH
        )
    for copy in fact_loads:
        copy.start()
    for ch in range(CHUNKS):
        for copy in loads(ch):
            copy.start()
    for copy in fact_loads:
        copy.wait()

    local_prompt = jnp.bitwise_and(facts[0], SLOTS - 1)
    rows = lax.broadcasted_iota(jnp.int32, (SLOTS, SLOTS), 0)
    lanes = lax.broadcasted_iota(jnp.int32, (SLOTS, SLOTS), 1)
    hot = jnp.where(rows == local_prompt, 1.0, 0.0).astype(jnp.bfloat16)
    for part in range(3):
        one_hot3[:, part * SLOTS : (part + 1) * SLOTS] = hot
    lens = facts[1].astype(jnp.float32)
    column = jnp.sum(jnp.where(rows == lanes, lens, 0.0), axis=1, keepdims=True)
    len_col[...] = jnp.broadcast_to(column, (SLOTS, LANES))
    sums[...] = jnp.zeros_like(sums)

    def compute(ch):
        for copy in loads(ch):
            copy.wait()

        @pl.loop(0, WIDTHS[ch] // UNIT)
        def _(unit):
            start = pl.multiple_of(STARTS[ch] + unit * UNIT, UNIT)

            @pl.loop(0, SLOTS // 16)
            def _(block):
                r0 = pl.multiple_of(block * 16, 16)
                length = len_col[pl.ds(r0, 16), :]
                s1 = sums[0, pl.ds(r0, 16), :]
                s2 = sums[1, pl.ds(r0, 16), :]
                lane = lax.broadcasted_iota(jnp.int32, (16, LANES), 1)
                for t in range(UNIT // LANES):
                    c0 = pl.multiple_of(start + t * LANES, LANES)
                    p = policy[pl.ds(r0, 16), pl.ds(c0, LANES)]
                    a = anchor[pl.ds(r0, 16), pl.ds(c0, LANES)]
                    valid = (lane + c0).astype(jnp.float32) < length
                    d = a - p
                    ratio = jnp.exp(d)
                    s1 = s1 + jnp.where(valid, p, 0.0)
                    s2 = s2 + jnp.where(valid, ratio - d - 1.0, 0.0)
                    for i, part in enumerate(parts_of(ratio)):
                        stack[pl.ds(pl.multiple_of(i * SLOTS + r0, 16), 16), t * LANES : (t + 1) * LANES] = part
                sums[0, pl.ds(r0, 16), :] = s1
                sums[1, pl.ds(r0, 16), :] = s2

            cols = pl.ds(start, UNIT)
            sent[:, cols] = jnp.dot(one_hot3[...], stack[...], preferred_element_type=jnp.float32)
            got[me, :, cols] = sent[pl.ds(pl.multiple_of(me * 16, 16), 16), cols]

    def copies(ch):
        for j, (dx, dy) in enumerate(OFFSETS):
            px, py = peer(dx, dy)
            first = pl.multiple_of((px * 4 + py) * 16, 16)
            yield pltpu.make_async_remote_copy(
                src_ref=sent.at[pl.ds(first, 16), columns(ch)],
                dst_ref=got.at[me, :, columns(ch)],
                send_sem=send_sem.at[ch, j],
                recv_sem=recv_sem.at[ch, j],
                device_id=(mz, mc, px, py),
                device_id_type=MESH,
            )

    def small_copies(source, target, sends, recvs):
        for j, (dx, dy) in enumerate(OFFSETS):
            px, py = peer(dx, dy)
            yield pltpu.make_async_remote_copy(
                src_ref=source.at[lax.div(px, 2)],
                dst_ref=target.at[me],
                send_sem=sends.at[j],
                recv_sem=recvs.at[j],
                device_id=(mz, mc, px, py),
                device_id_type=MESH,
            )

    def count_copies():
        for j, (dz, dc) in enumerate(GX_OFFSETS):
            yield pltpu.make_async_remote_copy(
                src_ref=count_out,
                dst_ref=count_in.at[me_gx],
                send_sem=count_send.at[j],
                recv_sem=count_recv.at[j],
                device_id=(lax.rem(mz + dz, 4), lax.rem(mc + dc, 2), mx, my),
                device_id_type=MESH,
            )

    compute(0)
    pl.semaphore_wait(barrier, len(OFFSETS) + len(GX_OFFSETS))
    for copy in copies(0):
        copy.start()

    hot = one_hot3[:, 0:SLOTS]
    lens = facts[1].astype(jnp.float32)
    rewards = facts[2].astype(jnp.float32) * 0.25
    which = lax.broadcasted_iota(jnp.int32, (8, SLOTS), 0)
    both = jnp.where(which == 0, lens, jnp.where(which == 1, rewards, 0.0))
    moved = picked(both, hot, 1)
    local_count = jnp.sum(lens, axis=1, keepdims=True)
    for half in range(2):
        at = half * LANES
        info_out[half, 0:2, :] = moved[0:2, at : at + LANES]
        info_out[half, 2:4, :] = jnp.broadcast_to(local_count, (2, LANES))

    compute(1)
    for copy in small_copies(info_out, info_in, info_send, info_recv):
        copy.start()
    for copy in copies(1):
        copy.start()
    for ch in range(2, CHUNKS):
        compute(ch)
        if ch == CHUNKS - 1:
            ones = jnp.ones((8, LANES), jnp.float32)
            across = (((1,), (1,)), ((), ()))
            row1, row2 = (
                lax.dot_general(
                    ones, sums[i], across, precision=lax.Precision.HIGHEST, preferred_element_type=jnp.float32
                )
                for i in range(2)
            )
            moved = picked(jnp.where(which == 0, row1, row2), hot, 1)
            for half in range(2):
                at = half * LANES
                sums_out[half] = moved[0:2, at : at + LANES]
            for copy in small_copies(sums_out, sums_in, sums_send, sums_recv):
                copy.start()
        for copy in copies(ch):
            copy.start()

    half = lax.div(mx, 2)
    info_in[me] = info_out[half]
    sums_in[me] = sums_out[half]
    for copy in small_copies(info_out, info_in, info_send, info_recv):
        copy.wait()
    count = info_in[0, 2:3, :]
    for k in range(1, MEMBERS):
        count = count + info_in[k, 2:3, :]
    count_out[...] = count
    count_in[me_gx] = count
    for copy in count_copies():
        copy.start()

    total = info_in[0, 1:2, :]
    for k in range(1, MEMBERS):
        total = total + info_in[k, 1:2, :]
    lane = lax.broadcasted_iota(jnp.int32, (16, LANES), 1)
    row = lax.broadcasted_iota(jnp.int32, (16, LANES), 0)
    mine = lane == lax.rem(me, 8) * 16 + row

    def to_column(line):
        return jnp.broadcast_to(jnp.sum(jnp.where(mine, line, 0.0), axis=1, keepdims=True), (16, LANES))

    for k in range(MEMBERS):
        advantage = (MEMBERS * info_in[k, 1:2, :] - total) / (MEMBERS - 1)
        len_in[k] = to_column(info_in[k, 0:1, :])
        adv_in[k] = to_column(advantage)

    for copy in count_copies():
        copy.wait()
    tokens = count_in[0]
    for g in range(1, 8):
        tokens = tokens + count_in[g]
    grad_scale = SAMPLES * TOKENS / tokens
    loss_scale = SAMPLES / tokens

    for ch in range(CHUNKS):
        if ch == CHUNKS - 1:
            for copy in small_copies(sums_out, sums_in, sums_send, sums_recv):
                copy.wait()
            member = lax.broadcasted_iota(jnp.int32, (MEMBERS, LANES), 0)
            adv_rows = jnp.zeros((MEMBERS, LANES), jnp.float32)
            loss_rows = jnp.zeros((MEMBERS, LANES), jnp.float32)
            for k in range(MEMBERS):
                advantage = (MEMBERS * info_in[k, 1:2, :] - total) / (MEMBERS - 1)
                loss = (KL * sums_in[k, 1:2, :] - advantage * sums_in[k, 0:1, :]) * loss_scale
                adv_rows = jnp.where(member == k, advantage, adv_rows)
                loss_rows = jnp.where(member == k, loss, loss_rows)
            select = jnp.where(mine, 1.0, 0.0).astype(jnp.bfloat16)
            loss_ref[...] = picked(loss_rows, select, 1)
            adv_ref[...] = picked(adv_rows, select, 1)
            for earlier in range(CHUNKS - 1):
                for copy in copies(earlier):
                    copy.wait_send()
        for copy in copies(ch):
            copy.wait_recv()

        @pl.loop(0, MEMBERS)
        def _(k):
            length = len_in[k]
            advantage = adv_in[k]
            for t in range(WIDTHS[ch] // LANES):
                c0 = STARTS[ch] + t * LANES
                ratio = got[k, :, c0 : c0 + LANES]
                valid = (lane + c0).astype(jnp.float32) < length
                grad_ref[k, :, c0 : c0 + LANES] = (
                    jnp.where(valid, KL * (1.0 - ratio) - advantage, 0.0) * grad_scale
                )

    for copy in copies(CHUNKS - 1):
        copy.wait_send()


def put_out(grad, loss, adv, grad_out, loss_out, adv_out, sem):
    moves = [
        pltpu.make_async_copy(source, target, sem.at[i])
        for i, (source, target) in enumerate(((loss, loss_out), (adv, adv_out)))
    ]
    pieces = 4
    each = MEMBERS // pieces
    for i in range(pieces):
        part = pl.ds(i * each, each)
        moves.append(pltpu.make_async_copy(grad.at[part], grad_out.at[part], sem.at[2 + i]))
    for move in moves:
        move.start()
    for move in moves:
        move.wait()


def body(policy_logp, anchor_logp, lengths, rewards, slot_prompt):
    f32, bf16, dma = jnp.float32, jnp.bfloat16, pltpu.SemaphoreType.DMA
    n = len(OFFSETS)
    vmem = pl.BlockSpec(memory_space=pltpu.VMEM)
    hbm = pl.BlockSpec(memory_space=pl.ANY)
    results = pl.pallas_call(
        kernel,
        out_shape=(
            pltpu.VMEM((MEMBERS, 16, TOKENS), f32),
            pltpu.VMEM((MEMBERS, 16), f32),
            pltpu.VMEM((MEMBERS, 16), f32),
        ),
        in_specs=[hbm] * 5,
        out_specs=(vmem, vmem, vmem),
        scratch_shapes=[
            pltpu.VMEM((SLOTS, TOKENS), f32),
            pltpu.VMEM((SLOTS, TOKENS), f32),
            pltpu.VMEM((3, 1, SLOTS), jnp.int32),
            pltpu.VMEM((3 * SLOTS, UNIT), bf16),
            pltpu.VMEM((SLOTS, 3 * SLOTS), bf16),
            pltpu.VMEM((SLOTS, TOKENS), f32),
            pltpu.VMEM((MEMBERS, 16, TOKENS), f32),
            pltpu.VMEM((2, SLOTS, LANES), f32),
            pltpu.VMEM((SLOTS, LANES), f32),
            pltpu.VMEM((2, 4, LANES), f32),
            pltpu.VMEM((MEMBERS, 4, LANES), f32),
            pltpu.VMEM((2, 2, LANES), f32),
            pltpu.VMEM((MEMBERS, 2, LANES), f32),
            pltpu.VMEM((1, LANES), f32),
            pltpu.VMEM((8, 1, LANES), f32),
            pltpu.VMEM((MEMBERS, 16, LANES), f32),
            pltpu.VMEM((MEMBERS, 16, LANES), f32),
            dma((2, CHUNKS)), dma((3,)), dma((CHUNKS, n)), dma((CHUNKS, n)),
            dma((n,)), dma((n,)), dma((n,)), dma((n,)),
            dma((len(GX_OFFSETS),)), dma((len(GX_OFFSETS),)),
        ],
        compiler_params=pltpu.CompilerParams(
            collective_id=0, has_side_effects=True, vmem_limit_bytes=50 * 2**20
        ),
    )(policy_logp.reshape(SLOTS, TOKENS), anchor_logp.reshape(SLOTS, TOKENS), lengths, rewards, slot_prompt)
    return pl.pallas_call(
        put_out,
        out_shape=(
            jax.ShapeDtypeStruct((MEMBERS, 16, TOKENS), f32),
            jax.ShapeDtypeStruct((MEMBERS, 16), f32),
            jax.ShapeDtypeStruct((MEMBERS, 16), f32),
        ),
        in_specs=[vmem] * 3,
        out_specs=(hbm, hbm, hbm),
        scratch_shapes=[dma((6,))],
        compiler_params=pltpu.CompilerParams(vmem_limit_bytes=2**20),
    )(*(pltpu.with_memory_space_constraint(r, pltpu.VMEM) for r in results))


def solution(mesh):
    torus = Mesh(mesh.devices.reshape(4, 2, 4, 4), ("gx_0", "gx_1", "gy_0", "gy_1"))
    return jax.shard_map(
        body,
        mesh=torus,
        in_specs=(P(GY, GX, None), P(GY, GX, None), P(GY, GX), P(GY, GX), P(GY, GX)),
        out_specs=(P(None, GX_GY, None), P(None, GX_GY), P(None, GX_GY)),
        check_vma=False,
    )
```

```python
import functools

import jax
import jax.numpy as jnp
from jax import lax
from jax.experimental import pallas as pl
from jax.experimental.pallas import tpu as pltpu
from jax.sharding import Mesh
from jax.sharding import PartitionSpec as P

GX_GY = ("gx_0", "gx_1", "gy_0", "gy_1")
GY = ("gy_0", "gy_1")
GX = ("gx_0", "gx_1")
MESH = pl.DeviceIdType.MESH

MEMBERS = 16
SLOTS = 256
TOKENS = 4096
SAMPLES = 32768
KL = 0.1
LANES = 128
UNIT = 256
BLOCK = 64
WIDTHS = (512, 1024, 1536, 1024)
STARTS = tuple(sum(WIDTHS[:i]) for i in range(len(WIDTHS)))
CHUNKS = len(WIDTHS)

OFFSETS = (
    (2, 2), (2, 1), (1, 2), (2, 3), (3, 2), (1, 1), (3, 3), (1, 3),
    (3, 1), (0, 2), (2, 0), (0, 1), (1, 0), (0, 3), (3, 0),
)
GX_OFFSETS = ((2, 1), (2, 0), (1, 1), (3, 1), (1, 0), (3, 0), (0, 1))


def parts_of(x):
    high = x.astype(jnp.bfloat16)
    rest = x - high.astype(jnp.float32)
    mid = rest.astype(jnp.bfloat16)
    low = (rest - mid.astype(jnp.float32)).astype(jnp.bfloat16)
    return high, mid, low


def picked(x, one_hot, contract):
    dims = (((1,), (contract,)), ((), ()))
    high, mid, low = (
        lax.dot_general(part, one_hot, dims, preferred_element_type=jnp.float32)
        for part in parts_of(x)
    )
    return (high + mid) + low


def kernel(
    policy_hbm, anchor_hbm, len_hbm, reward_hbm, prompt_hbm,
    grad_ref, loss_ref, adv_ref,
    policy, anchor, facts, stack, one_hot3, sent, got, sums, len_col,
    info_out, info_in, sums_out, sums_in, count_out, count_in, total_out, total_in, len_in, adv_in,
    load_sem, facts_sem, send_sem, recv_sem,
    info_send, info_recv, sums_send, sums_recv, count_send, count_recv,
    total_send, total_recv,
):
    mz, mc = lax.axis_index("gx_0"), lax.axis_index("gx_1")
    mx, my = lax.axis_index("gy_0"), lax.axis_index("gy_1")
    me = mx * 4 + my
    me_gx = mz * 2 + mc

    def peer(dx, dy):
        return lax.rem(mx + dx, 4), lax.rem(my + dy, 4)

    def columns(ch):
        return pl.ds(STARTS[ch], WIDTHS[ch])

    def loads(ch):
        cols = columns(ch)
        return (
            pltpu.make_async_copy(policy_hbm.at[:, cols], policy.at[:, cols], load_sem.at[0, ch]),
            pltpu.make_async_copy(anchor_hbm.at[:, cols], anchor.at[:, cols], load_sem.at[1, ch]),
        )

    fact_loads = [
        pltpu.make_async_copy(source, facts.at[i], facts_sem.at[i])
        for i, source in enumerate((prompt_hbm, len_hbm, reward_hbm))
    ]

    fact_loads[0].start()
    for copy in loads(0):
        copy.start()
    barrier = pltpu.get_barrier_semaphore()
    for dx, dy in OFFSETS:
        px, py = peer(dx, dy)
        pl.semaphore_signal(barrier, inc=1, device_id=(mz, mc, px, py), device_id_type=MESH)

    @pl.when(me == 0)
    def _():
        for dz, dc in GX_OFFSETS:
            pl.semaphore_signal(
                barrier, inc=1, device_id=(lax.rem(mz + dz, 4), lax.rem(mc + dc, 2), mx, my), device_id_type=MESH
            )

    for copy in fact_loads[1:]:
        copy.start()
    for ch in range(1, CHUNKS):
        for copy in loads(ch):
            copy.start()
    fact_loads[0].wait()

    local_prompt = jnp.bitwise_and(facts[0], SLOTS - 1)
    rows = lax.broadcasted_iota(jnp.int32, (SLOTS, SLOTS), 0)
    hot = jnp.where(rows == local_prompt, 1.0, 0.0).astype(jnp.bfloat16)
    for part in range(3):
        one_hot3[:, part * SLOTS : (part + 1) * SLOTS] = hot
    def compute(ch):
        for copy in loads(ch):
            copy.wait()

        unit = min(UNIT, WIDTHS[ch])

        @pl.loop(0, WIDTHS[ch] // unit)
        def _(step):
            start = pl.multiple_of(STARTS[ch] + step * unit, unit)

            @pl.loop(0, SLOTS // BLOCK)
            def _(block):
                r0 = pl.multiple_of(block * BLOCK, BLOCK)
                at, cols = pl.ds(r0, BLOCK), pl.ds(start, unit)
                ratio = jnp.exp(anchor[at, cols] - policy[at, cols])
                for i, part in enumerate(parts_of(ratio)):
                    stack[pl.ds(pl.multiple_of(i * SLOTS + r0, BLOCK), BLOCK), 0:unit] = part

            cols = pl.ds(start, unit)
            sent[:, cols] = jnp.dot(one_hot3[...], stack[:, 0:unit], preferred_element_type=jnp.float32)
            got[me, :, cols] = sent[pl.ds(pl.multiple_of(me * 16, 16), 16), cols]

    def add_sums(ch):
        @pl.loop(0, SLOTS // 32)
        def _(block):
            at = pl.ds(pl.multiple_of(block * 32, 32), 32)
            length = len_col[at, :]
            lane = lax.broadcasted_iota(jnp.int32, (32, LANES), 1)

            def add(t, so_far):
                s1, s2 = so_far
                c0 = pl.multiple_of(STARTS[ch] + t * LANES, LANES)
                p = policy[at, pl.ds(c0, LANES)]
                d = anchor[at, pl.ds(c0, LANES)] - p
                valid = (lane + c0).astype(jnp.float32) < length
                s1 = s1 + jnp.where(valid, p, 0.0)
                s2 = s2 + jnp.where(valid, jnp.exp(d) - d - 1.0, 0.0)
                return s1, s2

            sums[0, at, :], sums[1, at, :] = lax.fori_loop(
                0, WIDTHS[ch] // LANES, add, (sums[0, at, :], sums[1, at, :])
            )

    def copies(ch):
        for j, (dx, dy) in enumerate(OFFSETS):
            px, py = peer(dx, dy)
            first = pl.multiple_of((px * 4 + py) * 16, 16)
            yield pltpu.make_async_remote_copy(
                src_ref=sent.at[pl.ds(first, 16), columns(ch)],
                dst_ref=got.at[me, :, columns(ch)],
                send_sem=send_sem.at[ch, j],
                recv_sem=recv_sem.at[ch, j],
                device_id=(mz, mc, px, py),
                device_id_type=MESH,
            )

    def small_copies(source, target, sends, recvs):
        for j, (dx, dy) in enumerate(OFFSETS):
            px, py = peer(dx, dy)
            yield pltpu.make_async_remote_copy(
                src_ref=source.at[lax.div(px, 2)],
                dst_ref=target.at[me],
                send_sem=sends.at[j],
                recv_sem=recvs.at[j],
                device_id=(mz, mc, px, py),
                device_id_type=MESH,
            )

    def count_copies():
        for j, (dz, dc) in enumerate(GX_OFFSETS):
            yield pltpu.make_async_remote_copy(
                src_ref=count_out,
                dst_ref=count_in.at[me_gx],
                send_sem=count_send.at[j],
                recv_sem=count_recv.at[j],
                device_id=(lax.rem(mz + dz, 4), lax.rem(mc + dc, 2), mx, my),
                device_id_type=MESH,
            )

    def total_copies():
        for j, (dx, dy) in enumerate(OFFSETS):
            px, py = peer(dx, dy)
            yield pltpu.make_async_remote_copy(
                src_ref=total_out,
                dst_ref=total_in,
                send_sem=total_send.at[j],
                recv_sem=total_recv,
                device_id=(mz, mc, px, py),
                device_id_type=MESH,
            )

    def count_tokens():
        info_in[me] = info_out[lax.div(mx, 2)]
        for copy in small_copies(info_out, info_in, info_send, info_recv):
            copy.wait_recv()

        @pl.when(me == 0)
        def _():
            count = info_in[0, 2:3, :]
            for k in range(1, MEMBERS):
                count = count + info_in[k, 2:3, :]
            count_out[...] = count
            count_in[me_gx] = count
            for copy in count_copies():
                copy.start()
            for copy in count_copies():
                copy.wait_recv()
            tokens = count_in[0]
            for g in range(1, 8):
                tokens = tokens + count_in[g]
            total_out[...] = tokens
            total_in[...] = tokens
            for copy in total_copies():
                copy.start()

    compute(0)
    first = 1 - lax.min(me, 1)
    pl.semaphore_wait(barrier, len(OFFSETS) + len(GX_OFFSETS) * first)
    for copy in copies(0):
        copy.start()

    for copy in fact_loads[1:]:
        copy.wait()
    hot = one_hot3[:, 0:SLOTS]
    lens = facts[1].astype(jnp.float32)
    rewards = facts[2].astype(jnp.float32) * 0.25
    which = lax.broadcasted_iota(jnp.int32, (8, SLOTS), 0)
    both = jnp.where(which == 0, lens, jnp.where(which == 1, rewards, 0.0))
    moved = picked(both, hot, 1)
    local_count = jnp.sum(lens, axis=1, keepdims=True)
    for half in range(2):
        at = half * LANES
        info_out[half, 0:2, :] = moved[0:2, at : at + LANES]
        info_out[half, 2:4, :] = jnp.broadcast_to(local_count, (2, LANES))

    lanes = lax.broadcasted_iota(jnp.int32, (SLOTS, SLOTS), 1)
    column = jnp.sum(jnp.where(rows == lanes, lens, 0.0), axis=1, keepdims=True)
    len_col[...] = jnp.broadcast_to(column, (SLOTS, LANES))
    sums[...] = jnp.zeros_like(sums)

    compute(1)
    for copy in small_copies(info_out, info_in, info_send, info_recv):
        copy.start()
    for copy in copies(1):
        copy.start()
    for ch in range(2, CHUNKS):
        compute(ch)
        if ch == CHUNKS - 1:
            for each in range(CHUNKS):
                add_sums(each)
            ones = jnp.ones((8, LANES), jnp.float32)
            across = (((1,), (1,)), ((), ()))
            row1, row2 = (
                lax.dot_general(
                    ones, sums[i], across, precision=lax.Precision.HIGHEST, preferred_element_type=jnp.float32
                )
                for i in range(2)
            )
            moved = picked(jnp.where(which == 0, row1, row2), hot, 1)
            for half in range(2):
                at = half * LANES
                sums_out[half] = moved[0:2, at : at + LANES]
            for copy in small_copies(sums_out, sums_in, sums_send, sums_recv):
                copy.start()
        for copy in copies(ch):
            copy.start()
        if ch == 2:
            count_tokens()

    total = info_in[0, 1:2, :]
    for k in range(1, MEMBERS):
        total = total + info_in[k, 1:2, :]
    lane = lax.broadcasted_iota(jnp.int32, (16, LANES), 1)
    row = lax.broadcasted_iota(jnp.int32, (16, LANES), 0)
    mine = lane == lax.rem(me, 8) * 16 + row

    def to_column(line):
        return jnp.broadcast_to(jnp.sum(jnp.where(mine, line, 0.0), axis=1, keepdims=True), (16, LANES))

    for k in range(MEMBERS):
        advantage = (MEMBERS * info_in[k, 1:2, :] - total) / (MEMBERS - 1)
        len_in[k] = to_column(info_in[k, 0:1, :])
        adv_in[k] = to_column(advantage)

    @pl.when(me != 0)
    def _():
        next(total_copies()).wait_recv()

    tokens = total_in[...]
    grad_scale = SAMPLES * TOKENS / tokens
    loss_scale = SAMPLES / tokens

    for ch in range(CHUNKS):
        if ch == CHUNKS - 1:
            sums_in[me] = sums_out[lax.div(mx, 2)]
            for copy in small_copies(sums_out, sums_in, sums_send, sums_recv):
                copy.wait()
            member = lax.broadcasted_iota(jnp.int32, (MEMBERS, LANES), 0)
            adv_rows = jnp.zeros((MEMBERS, LANES), jnp.float32)
            loss_rows = jnp.zeros((MEMBERS, LANES), jnp.float32)
            for k in range(MEMBERS):
                advantage = (MEMBERS * info_in[k, 1:2, :] - total) / (MEMBERS - 1)
                loss = (KL * sums_in[k, 1:2, :] - advantage * sums_in[k, 0:1, :]) * loss_scale
                adv_rows = jnp.where(member == k, advantage, adv_rows)
                loss_rows = jnp.where(member == k, loss, loss_rows)
            select = jnp.where(mine, 1.0, 0.0).astype(jnp.bfloat16)
            loss_ref[...] = picked(loss_rows, select, 1)
            adv_ref[...] = picked(adv_rows, select, 1)
            for copy in small_copies(info_out, info_in, info_send, info_recv):
                copy.wait_send()

            @pl.when(me == 0)
            def _():
                for copy in (*count_copies(), *total_copies()):
                    copy.wait_send()

            for earlier in range(CHUNKS - 1):
                for copy in copies(earlier):
                    copy.wait_send()
        for copy in copies(ch):
            copy.wait_recv()

        @pl.loop(0, MEMBERS)
        def _(k):
            length = len_in[k]
            advantage = adv_in[k]
            for t in range(WIDTHS[ch] // LANES):
                c0 = STARTS[ch] + t * LANES
                ratio = got[k, :, c0 : c0 + LANES]
                valid = (lane + c0).astype(jnp.float32) < length
                grad_ref[k, :, c0 : c0 + LANES] = (
                    jnp.where(valid, KL * (1.0 - ratio) - advantage, 0.0) * grad_scale
                )

    for copy in copies(CHUNKS - 1):
        copy.wait_send()


def put_out(grad, loss, adv, grad_out, loss_out, adv_out, sem):
    moves = [
        pltpu.make_async_copy(source, target, sem.at[i])
        for i, (source, target) in enumerate(((loss, loss_out), (adv, adv_out)))
    ]
    pieces = 4
    each = MEMBERS // pieces
    for i in range(pieces):
        part = pl.ds(i * each, each)
        moves.append(pltpu.make_async_copy(grad.at[part], grad_out.at[part], sem.at[2 + i]))
    for move in moves:
        move.start()
    for move in moves:
        move.wait()


def body(policy_logp, anchor_logp, lengths, rewards, slot_prompt):
    f32, bf16, dma = jnp.float32, jnp.bfloat16, pltpu.SemaphoreType.DMA
    n = len(OFFSETS)
    vmem = pl.BlockSpec(memory_space=pltpu.VMEM)
    hbm = pl.BlockSpec(memory_space=pl.ANY)
    results = pl.pallas_call(
        kernel,
        out_shape=(
            pltpu.VMEM((MEMBERS, 16, TOKENS), f32),
            pltpu.VMEM((MEMBERS, 16), f32),
            pltpu.VMEM((MEMBERS, 16), f32),
        ),
        in_specs=[hbm] * 5,
        out_specs=(vmem, vmem, vmem),
        scratch_shapes=[
            pltpu.VMEM((SLOTS, TOKENS), f32),
            pltpu.VMEM((SLOTS, TOKENS), f32),
            pltpu.VMEM((3, 1, SLOTS), jnp.int32),
            pltpu.VMEM((3 * SLOTS, UNIT), bf16),
            pltpu.VMEM((SLOTS, 3 * SLOTS), bf16),
            pltpu.VMEM((SLOTS, TOKENS), f32),
            pltpu.VMEM((MEMBERS, 16, TOKENS), f32),
            pltpu.VMEM((2, SLOTS, LANES), f32),
            pltpu.VMEM((SLOTS, LANES), f32),
            pltpu.VMEM((2, 4, LANES), f32),
            pltpu.VMEM((MEMBERS, 4, LANES), f32),
            pltpu.VMEM((2, 2, LANES), f32),
            pltpu.VMEM((MEMBERS, 2, LANES), f32),
            pltpu.VMEM((1, LANES), f32),
            pltpu.VMEM((8, 1, LANES), f32),
            pltpu.VMEM((1, LANES), f32),
            pltpu.VMEM((1, LANES), f32),
            pltpu.VMEM((MEMBERS, 16, LANES), f32),
            pltpu.VMEM((MEMBERS, 16, LANES), f32),
            dma((2, CHUNKS)), dma((3,)), dma((CHUNKS, n)), dma((CHUNKS, n)),
            dma((n,)), dma((n,)), dma((n,)), dma((n,)),
            dma((len(GX_OFFSETS),)), dma((len(GX_OFFSETS),)),
            dma((n,)), dma,
        ],
        compiler_params=pltpu.CompilerParams(
            collective_id=0, has_side_effects=True, vmem_limit_bytes=50 * 2**20
        ),
    )(policy_logp.reshape(SLOTS, TOKENS), anchor_logp.reshape(SLOTS, TOKENS), lengths, rewards, slot_prompt)
    return pl.pallas_call(
        put_out,
        out_shape=(
            jax.ShapeDtypeStruct((MEMBERS, 16, TOKENS), f32),
            jax.ShapeDtypeStruct((MEMBERS, 16), f32),
            jax.ShapeDtypeStruct((MEMBERS, 16), f32),
        ),
        in_specs=[vmem] * 3,
        out_specs=(hbm, hbm, hbm),
        scratch_shapes=[dma((6,))],
        compiler_params=pltpu.CompilerParams(vmem_limit_bytes=2**20),
    )(*(pltpu.with_memory_space_constraint(r, pltpu.VMEM) for r in results))


def solution(mesh):
    torus = Mesh(mesh.devices.reshape(4, 2, 4, 4), ("gx_0", "gx_1", "gy_0", "gy_1"))
    return jax.shard_map(
        body,
        mesh=torus,
        in_specs=(P(GY, GX, None), P(GY, GX, None), P(GY, GX), P(GY, GX), P(GY, GX)),
        out_specs=(P(None, GX_GY, None), P(None, GX_GY), P(None, GX_GY)),
        check_vma=False,
    )
```

```python
import functools

import jax
import jax.numpy as jnp
from jax import lax
from jax.experimental import pallas as pl
from jax.experimental.pallas import tpu as pltpu
from jax.sharding import Mesh
from jax.sharding import PartitionSpec as P

GX_GY = ("gx_0", "gx_1", "gy_0", "gy_1")
GY = ("gy_0", "gy_1")
GX = ("gx_0", "gx_1")
MESH = pl.DeviceIdType.MESH

MEMBERS = 16
SLOTS = 256
TOKENS = 4096
SAMPLES = 32768
KL = 0.1
LANES = 128
UNIT = 256
BLOCK = 64
WIDTHS = (512, 1024, 1536, 1024)
STARTS = tuple(sum(WIDTHS[:i]) for i in range(len(WIDTHS)))
CHUNKS = len(WIDTHS)
LOADS = (WIDTHS[0] // 2, WIDTHS[0] // 2, *WIDTHS[1:])

OFFSETS = (
    (2, 2), (2, 1), (1, 2), (2, 3), (3, 2), (1, 1), (3, 3), (1, 3),
    (3, 1), (0, 2), (2, 0), (0, 1), (1, 0), (0, 3), (3, 0),
)
GX_OFFSETS = ((2, 1), (2, 0), (1, 1), (3, 1), (1, 0), (3, 0), (0, 1))


def parts_of(x):
    high = x.astype(jnp.bfloat16)
    rest = x - high.astype(jnp.float32)
    mid = rest.astype(jnp.bfloat16)
    low = (rest - mid.astype(jnp.float32)).astype(jnp.bfloat16)
    return high, mid, low


def picked(x, one_hot, contract):
    dims = (((1,), (contract,)), ((), ()))
    high, mid, low = (
        lax.dot_general(part, one_hot, dims, preferred_element_type=jnp.float32)
        for part in parts_of(x)
    )
    return (high + mid) + low


def kernel(
    policy_hbm, anchor_hbm, len_hbm, reward_hbm, prompt_hbm,
    grad_ref, loss_ref, adv_ref,
    policy, anchor, facts, stack, one_hot3, sent, got, sums, len_col,
    info_out, info_in, sums_out, sums_in, count_out, count_in, total_out, total_in, len_in, adv_in,
    load_sem, facts_sem, send_sem, recv_sem,
    info_send, info_recv, sums_send, sums_recv, count_send, count_recv,
    total_send, total_recv,
):
    mz, mc = lax.axis_index("gx_0"), lax.axis_index("gx_1")
    mx, my = lax.axis_index("gy_0"), lax.axis_index("gy_1")
    me = mx * 4 + my
    me_gx = mz * 2 + mc

    def peer(dx, dy):
        return lax.rem(mx + dx, 4), lax.rem(my + dy, 4)

    def columns(ch):
        return pl.ds(STARTS[ch], WIDTHS[ch])

    def loads(part):
        cols = pl.ds(sum(LOADS[:part]), LOADS[part])
        return (
            pltpu.make_async_copy(policy_hbm.at[:, cols], policy.at[:, cols], load_sem.at[0, part]),
            pltpu.make_async_copy(anchor_hbm.at[:, cols], anchor.at[:, cols], load_sem.at[1, part]),
        )

    fact_loads = [
        pltpu.make_async_copy(source, facts.at[i], facts_sem.at[i])
        for i, source in enumerate((prompt_hbm, len_hbm, reward_hbm))
    ]

    fact_loads[0].start()
    for copy in loads(0):
        copy.start()
    barrier = pltpu.get_barrier_semaphore()
    for dx, dy in OFFSETS:
        px, py = peer(dx, dy)
        pl.semaphore_signal(barrier, inc=1, device_id=(mz, mc, px, py), device_id_type=MESH)

    @pl.when(me == 0)
    def _():
        for dz, dc in GX_OFFSETS:
            pl.semaphore_signal(
                barrier, inc=1, device_id=(lax.rem(mz + dz, 4), lax.rem(mc + dc, 2), mx, my), device_id_type=MESH
            )

    for copy in fact_loads[1:]:
        copy.start()
    for part in range(1, len(LOADS)):
        for copy in loads(part):
            copy.start()
    fact_loads[0].wait()

    local_prompt = jnp.bitwise_and(facts[0], SLOTS - 1)
    rows = lax.broadcasted_iota(jnp.int32, (SLOTS, SLOTS), 0)
    hot = jnp.where(rows == local_prompt, 1.0, 0.0).astype(jnp.bfloat16)
    for part in range(3):
        one_hot3[:, part * SLOTS : (part + 1) * SLOTS] = hot
    def compute(part):
        for copy in loads(part):
            copy.wait()

        unit = min(UNIT, LOADS[part])

        @pl.loop(0, LOADS[part] // unit)
        def _(step):
            start = pl.multiple_of(sum(LOADS[:part]) + step * unit, unit)

            @pl.loop(0, SLOTS // BLOCK)
            def _(block):
                r0 = pl.multiple_of(block * BLOCK, BLOCK)
                at, cols = pl.ds(r0, BLOCK), pl.ds(start, unit)
                ratio = jnp.exp(anchor[at, cols] - policy[at, cols])
                for i, piece in enumerate(parts_of(ratio)):
                    stack[pl.ds(pl.multiple_of(i * SLOTS + r0, BLOCK), BLOCK), 0:unit] = piece

            cols = pl.ds(start, unit)
            sent[:, cols] = jnp.dot(one_hot3[...], stack[:, 0:unit], preferred_element_type=jnp.float32)
            got[me, :, cols] = sent[pl.ds(pl.multiple_of(me * 16, 16), 16), cols]

    def add_sums(ch):
        @pl.loop(0, SLOTS // 32)
        def _(block):
            at = pl.ds(pl.multiple_of(block * 32, 32), 32)
            length = len_col[at, :]
            lane = lax.broadcasted_iota(jnp.int32, (32, LANES), 1)

            def add(t, so_far):
                s1, s2 = so_far
                c0 = pl.multiple_of(STARTS[ch] + t * LANES, LANES)
                p = policy[at, pl.ds(c0, LANES)]
                d = anchor[at, pl.ds(c0, LANES)] - p
                valid = (lane + c0).astype(jnp.float32) < length
                s1 = s1 + jnp.where(valid, p, 0.0)
                s2 = s2 + jnp.where(valid, jnp.exp(d) - d - 1.0, 0.0)
                return s1, s2

            sums[0, at, :], sums[1, at, :] = lax.fori_loop(
                0, WIDTHS[ch] // LANES, add, (sums[0, at, :], sums[1, at, :])
            )

    def copies(ch):
        for j, (dx, dy) in enumerate(OFFSETS):
            px, py = peer(dx, dy)
            first = pl.multiple_of((px * 4 + py) * 16, 16)
            yield pltpu.make_async_remote_copy(
                src_ref=sent.at[pl.ds(first, 16), columns(ch)],
                dst_ref=got.at[me, :, columns(ch)],
                send_sem=send_sem.at[ch, j],
                recv_sem=recv_sem.at[ch, j],
                device_id=(mz, mc, px, py),
                device_id_type=MESH,
            )

    def small_copies(source, target, sends, recvs):
        for j, (dx, dy) in enumerate(OFFSETS):
            px, py = peer(dx, dy)
            yield pltpu.make_async_remote_copy(
                src_ref=source.at[lax.div(px, 2)],
                dst_ref=target.at[me],
                send_sem=sends.at[j],
                recv_sem=recvs.at[j],
                device_id=(mz, mc, px, py),
                device_id_type=MESH,
            )

    def count_copies():
        for j, (dz, dc) in enumerate(GX_OFFSETS):
            yield pltpu.make_async_remote_copy(
                src_ref=count_out,
                dst_ref=count_in.at[me_gx],
                send_sem=count_send.at[j],
                recv_sem=count_recv.at[j],
                device_id=(lax.rem(mz + dz, 4), lax.rem(mc + dc, 2), mx, my),
                device_id_type=MESH,
            )

    def total_copies():
        for j, (dx, dy) in enumerate(OFFSETS):
            px, py = peer(dx, dy)
            yield pltpu.make_async_remote_copy(
                src_ref=total_out,
                dst_ref=total_in,
                send_sem=total_send.at[j],
                recv_sem=total_recv,
                device_id=(mz, mc, px, py),
                device_id_type=MESH,
            )

    def count_tokens():
        info_in[me] = info_out[lax.div(mx, 2)]
        for copy in small_copies(info_out, info_in, info_send, info_recv):
            copy.wait_recv()

        @pl.when(me == 0)
        def _():
            count = info_in[0, 2:3, :]
            for k in range(1, MEMBERS):
                count = count + info_in[k, 2:3, :]
            count_out[...] = count
            count_in[me_gx] = count
            for copy in count_copies():
                copy.start()
            for copy in count_copies():
                copy.wait_recv()
            tokens = count_in[0]
            for g in range(1, 8):
                tokens = tokens + count_in[g]
            total_out[...] = tokens
            total_in[...] = tokens
            for copy in total_copies():
                copy.start()

    compute(0)
    compute(1)
    first = 1 - lax.min(me, 1)
    pl.semaphore_wait(barrier, len(OFFSETS) + len(GX_OFFSETS) * first)
    for copy in copies(0):
        copy.start()

    for copy in fact_loads[1:]:
        copy.wait()
    hot = one_hot3[:, 0:SLOTS]
    lens = facts[1].astype(jnp.float32)
    rewards = facts[2].astype(jnp.float32) * 0.25
    which = lax.broadcasted_iota(jnp.int32, (8, SLOTS), 0)
    both = jnp.where(which == 0, lens, jnp.where(which == 1, rewards, 0.0))
    moved = picked(both, hot, 1)
    local_count = jnp.sum(lens, axis=1, keepdims=True)
    for half in range(2):
        at = half * LANES
        info_out[half, 0:2, :] = moved[0:2, at : at + LANES]
        info_out[half, 2:4, :] = jnp.broadcast_to(local_count, (2, LANES))

    lanes = lax.broadcasted_iota(jnp.int32, (SLOTS, SLOTS), 1)
    column = jnp.sum(jnp.where(rows == lanes, lens, 0.0), axis=1, keepdims=True)
    len_col[...] = jnp.broadcast_to(column, (SLOTS, LANES))
    sums[...] = jnp.zeros_like(sums)

    compute(2)
    for copy in small_copies(info_out, info_in, info_send, info_recv):
        copy.start()
    for copy in copies(1):
        copy.start()
    for ch in range(2, CHUNKS):
        compute(ch + 1)
        if ch == CHUNKS - 1:
            for each in range(CHUNKS):
                add_sums(each)
            ones = jnp.ones((8, LANES), jnp.float32)
            across = (((1,), (1,)), ((), ()))
            row1, row2 = (
                lax.dot_general(
                    ones, sums[i], across, precision=lax.Precision.HIGHEST, preferred_element_type=jnp.float32
                )
                for i in range(2)
            )
            moved = picked(jnp.where(which == 0, row1, row2), hot, 1)
            for half in range(2):
                at = half * LANES
                sums_out[half] = moved[0:2, at : at + LANES]
            for copy in small_copies(sums_out, sums_in, sums_send, sums_recv):
                copy.start()
        for copy in copies(ch):
            copy.start()
        if ch == 2:
            count_tokens()

    total = info_in[0, 1:2, :]
    for k in range(1, MEMBERS):
        total = total + info_in[k, 1:2, :]
    lane = lax.broadcasted_iota(jnp.int32, (16, LANES), 1)
    row = lax.broadcasted_iota(jnp.int32, (16, LANES), 0)
    mine = lane == lax.rem(me, 8) * 16 + row

    def to_column(line):
        return jnp.broadcast_to(jnp.sum(jnp.where(mine, line, 0.0), axis=1, keepdims=True), (16, LANES))

    for k in range(MEMBERS):
        advantage = (MEMBERS * info_in[k, 1:2, :] - total) / (MEMBERS - 1)
        len_in[k] = to_column(info_in[k, 0:1, :])
        adv_in[k] = to_column(advantage)

    @pl.when(me != 0)
    def _():
        next(total_copies()).wait_recv()

    tokens = total_in[...]
    grad_scale = SAMPLES * TOKENS / tokens
    loss_scale = SAMPLES / tokens

    for ch in range(CHUNKS):
        if ch == CHUNKS - 1:
            sums_in[me] = sums_out[lax.div(mx, 2)]
            for copy in small_copies(sums_out, sums_in, sums_send, sums_recv):
                copy.wait()
            member = lax.broadcasted_iota(jnp.int32, (MEMBERS, LANES), 0)
            adv_rows = jnp.zeros((MEMBERS, LANES), jnp.float32)
            loss_rows = jnp.zeros((MEMBERS, LANES), jnp.float32)
            for k in range(MEMBERS):
                advantage = (MEMBERS * info_in[k, 1:2, :] - total) / (MEMBERS - 1)
                loss = (KL * sums_in[k, 1:2, :] - advantage * sums_in[k, 0:1, :]) * loss_scale
                adv_rows = jnp.where(member == k, advantage, adv_rows)
                loss_rows = jnp.where(member == k, loss, loss_rows)
            select = jnp.where(mine, 1.0, 0.0).astype(jnp.bfloat16)
            loss_ref[...] = picked(loss_rows, select, 1)
            adv_ref[...] = picked(adv_rows, select, 1)
            for copy in small_copies(info_out, info_in, info_send, info_recv):
                copy.wait_send()

            @pl.when(me == 0)
            def _():
                for copy in (*count_copies(), *total_copies()):
                    copy.wait_send()

            for earlier in range(CHUNKS - 1):
                for copy in copies(earlier):
                    copy.wait_send()
        def finish(k):
            length = len_in[k]
            advantage = adv_in[k]
            for t in range(WIDTHS[ch] // LANES):
                c0 = STARTS[ch] + t * LANES
                ratio = got[k, :, c0 : c0 + LANES]
                valid = (lane + c0).astype(jnp.float32) < length
                grad_ref[k, :, c0 : c0 + LANES] = (
                    jnp.where(valid, KL * (1.0 - ratio) - advantage, 0.0) * grad_scale
                )

        if ch == CHUNKS - 1:
            finish(me)
            for copy, (dx, dy) in zip(copies(ch), OFFSETS):
                copy.wait_recv()
                finish(lax.rem(mx + 4 - dx, 4) * 4 + lax.rem(my + 4 - dy, 4))
        else:
            for copy in copies(ch):
                copy.wait_recv()
            pl.loop(0, MEMBERS)(finish)

    for copy in copies(CHUNKS - 1):
        copy.wait_send()


def put_out(grad, loss, adv, grad_out, loss_out, adv_out, sem):
    moves = [
        pltpu.make_async_copy(source, target, sem.at[i])
        for i, (source, target) in enumerate(((loss, loss_out), (adv, adv_out)))
    ]
    pieces = 4
    each = MEMBERS // pieces
    for i in range(pieces):
        part = pl.ds(i * each, each)
        moves.append(pltpu.make_async_copy(grad.at[part], grad_out.at[part], sem.at[2 + i]))
    for move in moves:
        move.start()
    for move in moves:
        move.wait()


def body(policy_logp, anchor_logp, lengths, rewards, slot_prompt):
    f32, bf16, dma = jnp.float32, jnp.bfloat16, pltpu.SemaphoreType.DMA
    n = len(OFFSETS)
    vmem = pl.BlockSpec(memory_space=pltpu.VMEM)
    hbm = pl.BlockSpec(memory_space=pl.ANY)
    results = pl.pallas_call(
        kernel,
        out_shape=(
            pltpu.VMEM((MEMBERS, 16, TOKENS), f32),
            pltpu.VMEM((MEMBERS, 16), f32),
            pltpu.VMEM((MEMBERS, 16), f32),
        ),
        in_specs=[hbm] * 5,
        out_specs=(vmem, vmem, vmem),
        scratch_shapes=[
            pltpu.VMEM((SLOTS, TOKENS), f32),
            pltpu.VMEM((SLOTS, TOKENS), f32),
            pltpu.VMEM((3, 1, SLOTS), jnp.int32),
            pltpu.VMEM((3 * SLOTS, UNIT), bf16),
            pltpu.VMEM((SLOTS, 3 * SLOTS), bf16),
            pltpu.VMEM((SLOTS, TOKENS), f32),
            pltpu.VMEM((MEMBERS, 16, TOKENS), f32),
            pltpu.VMEM((2, SLOTS, LANES), f32),
            pltpu.VMEM((SLOTS, LANES), f32),
            pltpu.VMEM((2, 4, LANES), f32),
            pltpu.VMEM((MEMBERS, 4, LANES), f32),
            pltpu.VMEM((2, 2, LANES), f32),
            pltpu.VMEM((MEMBERS, 2, LANES), f32),
            pltpu.VMEM((1, LANES), f32),
            pltpu.VMEM((8, 1, LANES), f32),
            pltpu.VMEM((1, LANES), f32),
            pltpu.VMEM((1, LANES), f32),
            pltpu.VMEM((MEMBERS, 16, LANES), f32),
            pltpu.VMEM((MEMBERS, 16, LANES), f32),
            dma((2, len(LOADS))), dma((3,)), dma((CHUNKS, n)), dma((CHUNKS, n)),
            dma((n,)), dma((n,)), dma((n,)), dma((n,)),
            dma((len(GX_OFFSETS),)), dma((len(GX_OFFSETS),)),
            dma((n,)), dma,
        ],
        compiler_params=pltpu.CompilerParams(
            collective_id=0, has_side_effects=True, vmem_limit_bytes=50 * 2**20
        ),
    )(policy_logp.reshape(SLOTS, TOKENS), anchor_logp.reshape(SLOTS, TOKENS), lengths, rewards, slot_prompt)
    return pl.pallas_call(
        put_out,
        out_shape=(
            jax.ShapeDtypeStruct((MEMBERS, 16, TOKENS), f32),
            jax.ShapeDtypeStruct((MEMBERS, 16), f32),
            jax.ShapeDtypeStruct((MEMBERS, 16), f32),
        ),
        in_specs=[vmem] * 3,
        out_specs=(hbm, hbm, hbm),
        scratch_shapes=[dma((6,))],
        compiler_params=pltpu.CompilerParams(vmem_limit_bytes=2**20),
    )(*(pltpu.with_memory_space_constraint(r, pltpu.VMEM) for r in results))


def solution(mesh):
    torus = Mesh(mesh.devices.reshape(4, 2, 4, 4), ("gx_0", "gx_1", "gy_0", "gy_1"))
    return jax.shard_map(
        body,
        mesh=torus,
        in_specs=(P(GY, GX, None), P(GY, GX, None), P(GY, GX), P(GY, GX), P(GY, GX)),
        out_specs=(P(None, GX_GY, None), P(None, GX_GY), P(None, GX_GY)),
        check_vma=False,
    )
```

```python
import functools

import jax
import jax.numpy as jnp
from jax import lax
from jax.experimental import pallas as pl
from jax.experimental.pallas import tpu as pltpu
from jax.sharding import Mesh
from jax.sharding import PartitionSpec as P

GX_GY = ("gx_0", "gx_1", "gy_0", "gy_1")
GY = ("gy_0", "gy_1")
GX = ("gx_0", "gx_1")
MESH = pl.DeviceIdType.MESH

MEMBERS = 16
SLOTS = 256
TOKENS = 4096
SAMPLES = 32768
KL = 0.1
LANES = 128
UNIT = 256
BLOCK = 128
WIDTHS = (512, 1024, 1536, 1024)
STARTS = tuple(sum(WIDTHS[:i]) for i in range(len(WIDTHS)))
CHUNKS = len(WIDTHS)
LOADS = (WIDTHS[0] // 2, WIDTHS[0] // 2, *WIDTHS[1:])

OFFSETS = (
    (2, 2), (2, 1), (1, 2), (2, 3), (3, 2), (1, 1), (3, 3), (1, 3),
    (3, 1), (0, 2), (2, 0), (0, 1), (1, 0), (0, 3), (3, 0),
)
GX_OFFSETS = ((2, 1), (2, 0), (1, 1), (3, 1), (1, 0), (3, 0), (0, 1))


def parts_of(x):
    high = x.astype(jnp.bfloat16)
    rest = x - high.astype(jnp.float32)
    mid = rest.astype(jnp.bfloat16)
    low = (rest - mid.astype(jnp.float32)).astype(jnp.bfloat16)
    return high, mid, low


def picked(x, one_hot, contract):
    dims = (((1,), (contract,)), ((), ()))
    high, mid, low = (
        lax.dot_general(part, one_hot, dims, preferred_element_type=jnp.float32)
        for part in parts_of(x)
    )
    return (high + mid) + low


def kernel(
    policy_hbm, anchor_hbm, len_hbm, reward_hbm, prompt_hbm,
    grad_ref, loss_ref, adv_ref,
    policy, anchor, facts, stack, one_hot3, sent, got, sums, len_col,
    info_out, info_in, sums_out, sums_in, count_out, count_in, total_out, total_in, len_in, adv_in,
    load_sem, facts_sem, send_sem, recv_sem,
    info_send, info_recv, sums_send, sums_recv, count_send, count_recv,
    total_send, total_recv,
):
    mz, mc = lax.axis_index("gx_0"), lax.axis_index("gx_1")
    mx, my = lax.axis_index("gy_0"), lax.axis_index("gy_1")
    me = mx * 4 + my
    me_gx = mz * 2 + mc

    def peer(dx, dy):
        return lax.rem(mx + dx, 4), lax.rem(my + dy, 4)

    def columns(ch):
        return pl.ds(STARTS[ch], WIDTHS[ch])

    def loads(part):
        cols = pl.ds(sum(LOADS[:part]), LOADS[part])
        return (
            pltpu.make_async_copy(policy_hbm.at[:, cols], policy.at[:, cols], load_sem.at[0, part]),
            pltpu.make_async_copy(anchor_hbm.at[:, cols], anchor.at[:, cols], load_sem.at[1, part]),
        )

    fact_loads = [
        pltpu.make_async_copy(source, facts.at[i], facts_sem.at[i])
        for i, source in enumerate((prompt_hbm, len_hbm, reward_hbm))
    ]

    fact_loads[0].start()
    for copy in loads(0):
        copy.start()
    barrier = pltpu.get_barrier_semaphore()
    for dx, dy in OFFSETS:
        px, py = peer(dx, dy)
        pl.semaphore_signal(barrier, inc=1, device_id=(mz, mc, px, py), device_id_type=MESH)

    @pl.when(me == 0)
    def _():
        for dz, dc in GX_OFFSETS:
            pl.semaphore_signal(
                barrier, inc=1, device_id=(lax.rem(mz + dz, 4), lax.rem(mc + dc, 2), mx, my), device_id_type=MESH
            )

    for copy in fact_loads[1:]:
        copy.start()
    for part in range(1, len(LOADS)):
        for copy in loads(part):
            copy.start()
    fact_loads[0].wait()

    local_prompt = jnp.bitwise_and(facts[0], SLOTS - 1)
    rows = lax.broadcasted_iota(jnp.int32, (SLOTS, SLOTS), 0)
    hot = jnp.where(rows == local_prompt, 1.0, 0.0).astype(jnp.bfloat16)
    for part in range(3):
        one_hot3[:, part * SLOTS : (part + 1) * SLOTS] = hot
    def compute(part):
        for copy in loads(part):
            copy.wait()

        unit = min(UNIT, LOADS[part])

        @pl.loop(0, LOADS[part] // unit)
        def _(step):
            start = pl.multiple_of(sum(LOADS[:part]) + step * unit, unit)

            @pl.loop(0, SLOTS // BLOCK)
            def _(block):
                r0 = pl.multiple_of(block * BLOCK, BLOCK)
                at, cols = pl.ds(r0, BLOCK), pl.ds(start, unit)
                ratio = jnp.exp(anchor[at, cols] - policy[at, cols])
                for i, piece in enumerate(parts_of(ratio)):
                    stack[pl.ds(pl.multiple_of(i * SLOTS + r0, BLOCK), BLOCK), 0:unit] = piece

            cols = pl.ds(start, unit)
            sent[:, cols] = jnp.dot(one_hot3[...], stack[:, 0:unit], preferred_element_type=jnp.float32)
            got[me, :, cols] = sent[pl.ds(pl.multiple_of(me * 16, 16), 16), cols]

    def add_sums(ch):
        @pl.loop(0, SLOTS // 32)
        def _(block):
            at = pl.ds(pl.multiple_of(block * 32, 32), 32)
            length = len_col[at, :]
            lane = lax.broadcasted_iota(jnp.int32, (32, LANES), 1)

            def add(t, so_far):
                s1, s2 = so_far
                c0 = pl.multiple_of(STARTS[ch] + t * LANES, LANES)
                p = policy[at, pl.ds(c0, LANES)]
                d = anchor[at, pl.ds(c0, LANES)] - p
                valid = (lane + c0).astype(jnp.float32) < length
                s1 = s1 + jnp.where(valid, p, 0.0)
                s2 = s2 + jnp.where(valid, jnp.exp(d) - d - 1.0, 0.0)
                return s1, s2

            sums[0, at, :], sums[1, at, :] = lax.fori_loop(
                0, WIDTHS[ch] // LANES, add, (sums[0, at, :], sums[1, at, :])
            )

    def copies(ch):
        for j, (dx, dy) in enumerate(OFFSETS):
            px, py = peer(dx, dy)
            first = pl.multiple_of((px * 4 + py) * 16, 16)
            yield pltpu.make_async_remote_copy(
                src_ref=sent.at[pl.ds(first, 16), columns(ch)],
                dst_ref=got.at[me, :, columns(ch)],
                send_sem=send_sem.at[ch, j],
                recv_sem=recv_sem.at[ch, j],
                device_id=(mz, mc, px, py),
                device_id_type=MESH,
            )

    def small_copies(source, target, sends, recvs):
        for j, (dx, dy) in enumerate(OFFSETS):
            px, py = peer(dx, dy)
            yield pltpu.make_async_remote_copy(
                src_ref=source.at[lax.div(px, 2)],
                dst_ref=target.at[me],
                send_sem=sends.at[j],
                recv_sem=recvs.at[j],
                device_id=(mz, mc, px, py),
                device_id_type=MESH,
            )

    def count_copies():
        for j, (dz, dc) in enumerate(GX_OFFSETS):
            yield pltpu.make_async_remote_copy(
                src_ref=count_out,
                dst_ref=count_in.at[me_gx],
                send_sem=count_send.at[j],
                recv_sem=count_recv.at[j],
                device_id=(lax.rem(mz + dz, 4), lax.rem(mc + dc, 2), mx, my),
                device_id_type=MESH,
            )

    def total_copies():
        for j, (dx, dy) in enumerate(OFFSETS):
            px, py = peer(dx, dy)
            yield pltpu.make_async_remote_copy(
                src_ref=total_out,
                dst_ref=total_in,
                send_sem=total_send.at[j],
                recv_sem=total_recv,
                device_id=(mz, mc, px, py),
                device_id_type=MESH,
            )

    def count_tokens():
        info_in[me] = info_out[lax.div(mx, 2)]
        for copy in small_copies(info_out, info_in, info_send, info_recv):
            copy.wait_recv()

        @pl.when(me == 0)
        def _():
            count = info_in[0, 2:3, :]
            for k in range(1, MEMBERS):
                count = count + info_in[k, 2:3, :]
            count_out[...] = count
            count_in[me_gx] = count
            for copy in count_copies():
                copy.start()
            for copy in count_copies():
                copy.wait_recv()
            tokens = count_in[0]
            for g in range(1, 8):
                tokens = tokens + count_in[g]
            total_out[...] = tokens
            total_in[...] = tokens
            for copy in total_copies():
                copy.start()

    compute(0)
    compute(1)
    first = 1 - lax.min(me, 1)
    pl.semaphore_wait(barrier, len(OFFSETS) + len(GX_OFFSETS) * first)
    for copy in copies(0):
        copy.start()

    for copy in fact_loads[1:]:
        copy.wait()
    hot = one_hot3[:, 0:SLOTS]
    lens = facts[1].astype(jnp.float32)
    rewards = facts[2].astype(jnp.float32) * 0.25
    which = lax.broadcasted_iota(jnp.int32, (8, SLOTS), 0)
    both = jnp.where(which == 0, lens, jnp.where(which == 1, rewards, 0.0))
    moved = picked(both, hot, 1)
    local_count = jnp.sum(lens, axis=1, keepdims=True)
    for half in range(2):
        at = half * LANES
        info_out[half, 0:2, :] = moved[0:2, at : at + LANES]
        info_out[half, 2:4, :] = jnp.broadcast_to(local_count, (2, LANES))

    lanes = lax.broadcasted_iota(jnp.int32, (SLOTS, SLOTS), 1)
    column = jnp.sum(jnp.where(rows == lanes, lens, 0.0), axis=1, keepdims=True)
    len_col[...] = jnp.broadcast_to(column, (SLOTS, LANES))
    sums[...] = jnp.zeros_like(sums)

    compute(2)
    for copy in small_copies(info_out, info_in, info_send, info_recv):
        copy.start()
    for copy in copies(1):
        copy.start()
    for ch in range(2, CHUNKS):
        compute(ch + 1)
        if ch == CHUNKS - 1:
            for each in range(CHUNKS):
                add_sums(each)
            ones = jnp.ones((8, LANES), jnp.float32)
            across = (((1,), (1,)), ((), ()))
            row1, row2 = (
                lax.dot_general(
                    ones, sums[i], across, precision=lax.Precision.HIGHEST, preferred_element_type=jnp.float32
                )
                for i in range(2)
            )
            moved = picked(jnp.where(which == 0, row1, row2), hot, 1)
            for half in range(2):
                at = half * LANES
                sums_out[half] = moved[0:2, at : at + LANES]
            for copy in small_copies(sums_out, sums_in, sums_send, sums_recv):
                copy.start()
        for copy in copies(ch):
            copy.start()
        if ch == 2:
            count_tokens()

    total = info_in[0, 1:2, :]
    for k in range(1, MEMBERS):
        total = total + info_in[k, 1:2, :]
    lane = lax.broadcasted_iota(jnp.int32, (16, LANES), 1)
    row = lax.broadcasted_iota(jnp.int32, (16, LANES), 0)
    mine = lane == lax.rem(me, 8) * 16 + row

    def to_column(line):
        return jnp.broadcast_to(jnp.sum(jnp.where(mine, line, 0.0), axis=1, keepdims=True), (16, LANES))

    for k in range(MEMBERS):
        advantage = (MEMBERS * info_in[k, 1:2, :] - total) / (MEMBERS - 1)
        len_in[k] = to_column(info_in[k, 0:1, :])
        adv_in[k] = to_column(advantage)

    @pl.when(me != 0)
    def _():
        next(total_copies()).wait_recv()

    tokens = total_in[...]
    grad_scale = SAMPLES * TOKENS / tokens
    loss_scale = SAMPLES / tokens

    for ch in range(CHUNKS):
        if ch == CHUNKS - 1:
            sums_in[me] = sums_out[lax.div(mx, 2)]
            for copy in small_copies(sums_out, sums_in, sums_send, sums_recv):
                copy.wait()
            member = lax.broadcasted_iota(jnp.int32, (MEMBERS, LANES), 0)
            adv_rows = jnp.zeros((MEMBERS, LANES), jnp.float32)
            loss_rows = jnp.zeros((MEMBERS, LANES), jnp.float32)
            for k in range(MEMBERS):
                advantage = (MEMBERS * info_in[k, 1:2, :] - total) / (MEMBERS - 1)
                loss = (KL * sums_in[k, 1:2, :] - advantage * sums_in[k, 0:1, :]) * loss_scale
                adv_rows = jnp.where(member == k, advantage, adv_rows)
                loss_rows = jnp.where(member == k, loss, loss_rows)
            select = jnp.where(mine, 1.0, 0.0).astype(jnp.bfloat16)
            loss_ref[...] = picked(loss_rows, select, 1)
            adv_ref[...] = picked(adv_rows, select, 1)
            for copy in small_copies(info_out, info_in, info_send, info_recv):
                copy.wait_send()

            @pl.when(me == 0)
            def _():
                for copy in (*count_copies(), *total_copies()):
                    copy.wait_send()

            for earlier in range(CHUNKS - 1):
                for copy in copies(earlier):
                    copy.wait_send()
        def finish(k):
            length = len_in[k]
            advantage = adv_in[k]
            for t in range(WIDTHS[ch] // LANES):
                c0 = STARTS[ch] + t * LANES
                ratio = got[k, :, c0 : c0 + LANES]
                valid = (lane + c0).astype(jnp.float32) < length
                grad_ref[k, :, c0 : c0 + LANES] = (
                    jnp.where(valid, KL * (1.0 - ratio) - advantage, 0.0) * grad_scale
                )

        if ch == CHUNKS - 1:
            finish(me)
            for copy, (dx, dy) in zip(copies(ch), OFFSETS):
                copy.wait_recv()
                finish(lax.rem(mx + 4 - dx, 4) * 4 + lax.rem(my + 4 - dy, 4))
        else:
            for copy in copies(ch):
                copy.wait_recv()
            pl.loop(0, MEMBERS)(finish)

    for copy in copies(CHUNKS - 1):
        copy.wait_send()


def put_out(grad, loss, adv, grad_out, loss_out, adv_out, sem):
    moves = [
        pltpu.make_async_copy(source, target, sem.at[i])
        for i, (source, target) in enumerate(((loss, loss_out), (adv, adv_out)))
    ]
    pieces = 4
    each = MEMBERS // pieces
    for i in range(pieces):
        part = pl.ds(i * each, each)
        moves.append(pltpu.make_async_copy(grad.at[part], grad_out.at[part], sem.at[2 + i]))
    for move in moves:
        move.start()
    for move in moves:
        move.wait()


def body(policy_logp, anchor_logp, lengths, rewards, slot_prompt):
    f32, bf16, dma = jnp.float32, jnp.bfloat16, pltpu.SemaphoreType.DMA
    n = len(OFFSETS)
    vmem = pl.BlockSpec(memory_space=pltpu.VMEM)
    hbm = pl.BlockSpec(memory_space=pl.ANY)
    results = pl.pallas_call(
        kernel,
        out_shape=(
            pltpu.VMEM((MEMBERS, 16, TOKENS), f32),
            pltpu.VMEM((MEMBERS, 16), f32),
            pltpu.VMEM((MEMBERS, 16), f32),
        ),
        in_specs=[hbm] * 5,
        out_specs=(vmem, vmem, vmem),
        scratch_shapes=[
            pltpu.VMEM((SLOTS, TOKENS), f32),
            pltpu.VMEM((SLOTS, TOKENS), f32),
            pltpu.VMEM((3, 1, SLOTS), jnp.int32),
            pltpu.VMEM((3 * SLOTS, UNIT), bf16),
            pltpu.VMEM((SLOTS, 3 * SLOTS), bf16),
            pltpu.VMEM((SLOTS, TOKENS), f32),
            pltpu.VMEM((MEMBERS, 16, TOKENS), f32),
            pltpu.VMEM((2, SLOTS, LANES), f32),
            pltpu.VMEM((SLOTS, LANES), f32),
            pltpu.VMEM((2, 4, LANES), f32),
            pltpu.VMEM((MEMBERS, 4, LANES), f32),
            pltpu.VMEM((2, 2, LANES), f32),
            pltpu.VMEM((MEMBERS, 2, LANES), f32),
            pltpu.VMEM((1, LANES), f32),
            pltpu.VMEM((8, 1, LANES), f32),
            pltpu.VMEM((1, LANES), f32),
            pltpu.VMEM((1, LANES), f32),
            pltpu.VMEM((MEMBERS, 16, LANES), f32),
            pltpu.VMEM((MEMBERS, 16, LANES), f32),
            dma((2, len(LOADS))), dma((3,)), dma((CHUNKS, n)), dma((CHUNKS, n)),
            dma((n,)), dma((n,)), dma((n,)), dma((n,)),
            dma((len(GX_OFFSETS),)), dma((len(GX_OFFSETS),)),
            dma((n,)), dma,
        ],
        compiler_params=pltpu.CompilerParams(
            collective_id=0, has_side_effects=True, vmem_limit_bytes=50 * 2**20
        ),
    )(policy_logp.reshape(SLOTS, TOKENS), anchor_logp.reshape(SLOTS, TOKENS), lengths, rewards, slot_prompt)
    return pl.pallas_call(
        put_out,
        out_shape=(
            jax.ShapeDtypeStruct((MEMBERS, 16, TOKENS), f32),
            jax.ShapeDtypeStruct((MEMBERS, 16), f32),
            jax.ShapeDtypeStruct((MEMBERS, 16), f32),
        ),
        in_specs=[vmem] * 3,
        out_specs=(hbm, hbm, hbm),
        scratch_shapes=[dma((6,))],
        compiler_params=pltpu.CompilerParams(vmem_limit_bytes=2**20),
    )(*(pltpu.with_memory_space_constraint(r, pltpu.VMEM) for r in results))


def solution(mesh):
    torus = Mesh(mesh.devices.reshape(4, 2, 4, 4), ("gx_0", "gx_1", "gy_0", "gy_1"))
    return jax.shard_map(
        body,
        mesh=torus,
        in_specs=(P(GY, GX, None), P(GY, GX, None), P(GY, GX), P(GY, GX), P(GY, GX)),
        out_specs=(P(None, GX_GY, None), P(None, GX_GY), P(None, GX_GY)),
        check_vma=False,
    )
```
